32 devices in a mesh: row: 4 (over z), vec: 8 (over y, x, core).
Axes of the slice: x: 2, y: 2, z: 4, core: 2. Of those that a mesh axis runs over, the one named last changes fastest.
Arguments:
- vectors: float32 [4096, 4096], P('row', 'vec'), may hold values from -6 to 6
- block_index: int32 [3, 4], replicated, may hold values from 0 to 7
- block_offset: int32 [3, 4], replicated, may hold values from 0 to 3, as said below
- reflector_vectors: float32 [4, 8, 512, 256], P('row', 'vec'), may hold values from -0.25 to 0.25
- reflector_factors: float32 [4, 8, 256, 256], P('row', 'vec'), may hold values from -0.1875 to 0.1875
Outputs:
- updated: float32 [4096, 4096], P('row', 'vec')
The draws below stay inside these ranges and needn't reach their ends.
Inputs may be any that keep to these rules, and one draw needn't show every extreme that they name: `block_offset`: the last owner's offset is at most 2, so every block lies inside the slab.
All inputs are finite; a program needn't handle non-finite values.
Results may differ from the reference program's by a relative error of at most 0.0001.
Values sent between devices are 32-bit elements; how exact they have to be, the bound alone decides.
No kernel may reach another device: no remote copies, remote signals or barrier semaphores. Data moves between devices by JAX's collectives and lax.ppermute only.
A program may use at most 64 MiB of HBM per device.

```python
import jax
import jax.numpy as jnp
from jax import lax

ROW_DEV = 1024
REFL = 256
BLOCK_ROWS = 512
FRONTS = 3
NR = 4096
NV = 4096
POOL = 8
N_ROW = 4
N_VEC = 8


def draw_block_offset(key, part):
    slots = ROW_DEV // REFL
    first_key, second_key = jax.random.split(jax.random.fold_in(key, 11))
    base = jax.random.randint(first_key, (FRONTS, N_ROW), 0, slots)
    upper = jax.random.randint(second_key, (FRONTS, N_ROW), 0, 2)
    value = jnp.where(upper == 1, slots - 1, base)
    final = jnp.arange(N_ROW) == N_ROW - 1
    return jnp.where(final[None, :], jnp.minimum(value, slots - 2), value).astype(jnp.int32)


def place_ends(values, own_key, low, largest):
    longest = values.shape.index(max(values.shape))
    spots = []
    for shift in (0, 1):
        where = [jax.random.randint(jax.random.fold_in(own_key, axis), (), 0, length) for axis, length in enumerate(values.shape)]
        where[longest] = (where[longest] + shift) % values.shape[longest]
        spots.append(tuple(where))
    return values.at[spots[0]].set(low).at[spots[1]].set(largest)


def levels(rng, shape, pieces, low, high):
    loudness, own = 1.0, jax.random.fold_in(rng, 6)
    for axis_at, parts in pieces:
        draws = jnp.exp(jax.random.uniform(jax.random.fold_in(own, axis_at), (parts,), jnp.float32, low / len(pieces), high / len(pieces)))
        loudness = loudness * jnp.repeat(draws, shape[axis_at] // parts).reshape([-1 if axis == axis_at else 1 for axis in range(len(shape))])
    return loudness


def centred(own_key, dims, deviation, most, cuts=(), kind=jnp.bfloat16):
    result = deviation * jax.random.normal(own_key, dims, jnp.float32)
    if cuts:
        result = result * levels(own_key, dims, cuts, -0.22, 0.18)
    return jnp.clip(result, -most, most).astype(kind)


def setup_inputs(seed: int = 0) -> dict:
    arg_keys = jax.random.split(jax.random.key(seed), 6)
    vectors = centred(arg_keys[0], (NR, NV), 1.0, 6.0, ((0, 4), (1, 8)), jnp.float32)
    block_index = place_ends(jax.random.randint(arg_keys[1], (FRONTS, N_ROW), 0, N_VEC), jax.random.fold_in(arg_keys[1], 1), 0, N_VEC - 1).astype(jnp.int32)
    block_offset = draw_block_offset(jax.random.fold_in(arg_keys[5], 71), 0)
    reflector_vectors = centred(arg_keys[3], (N_ROW, POOL, BLOCK_ROWS, REFL), BLOCK_ROWS ** -0.5, 0.25, ((0, 4), (1, 8)), jnp.float32)
    reflector_factors = centred(arg_keys[4], (N_ROW, POOL, REFL, REFL), (4 * REFL) ** -0.5, 0.1875, ((0, 4), (1, 8)), jnp.float32)
    return {"vectors": vectors, "block_index": block_index, "block_offset": block_offset, "reflector_vectors": reflector_vectors, "reflector_factors": reflector_factors}


def apply_reflector_block(row_window, vector_matrix, triangular_matrix):
    high_precision = lax.Precision.HIGHEST
    inner_product = jnp.dot(vector_matrix.T, row_window, precision=high_precision, preferred_element_type=jnp.float32)
    mixed_rows = jnp.dot(jnp.triu(triangular_matrix), inner_product, precision=high_precision, preferred_element_type=jnp.float32)
    return row_window - jnp.dot(vector_matrix, mixed_rows, precision=high_precision, preferred_element_type=jnp.float32)


def reference(vectors, block_index, block_offset, reflector_vectors, reflector_factors):
    def one_block(step, row_slab):
        front = step // N_ROW
        owner_index = step % N_ROW
        select_block = block_index[front, owner_index]
        vector_matrix = reflector_vectors[owner_index, select_block]
        triangular_matrix = reflector_factors[owner_index, select_block]
        start_row = (owner_index * ROW_DEV + block_offset[front, owner_index] * REFL).astype(jnp.int32)
        row_window = lax.dynamic_slice_in_dim(row_slab, start_row, BLOCK_ROWS, 0)
        return lax.dynamic_update_slice_in_dim(row_slab, apply_reflector_block(row_window, vector_matrix, triangular_matrix), start_row, 0)

    return lax.fori_loop(0, FRONTS * N_ROW, one_block, vectors)
```

```python
import functools

import jax
import jax.numpy as jnp
from jax import lax
from jax.experimental import pallas as pl
from jax.experimental.pallas import tpu as pltpu
from jax.sharding import PartitionSpec as P

FRONTS = 3
CHUNKS = 2


F32 = jnp.float32
BF16 = jnp.bfloat16
VMEM = pl.BlockSpec(memory_space=pltpu.VMEM)
LIMIT = pltpu.CompilerParams(vmem_limit_bytes=12 << 20)
SMEM = pl.BlockSpec(memory_space=pltpu.SMEM)


def halves(value):
    high = value.astype(BF16)
    return high, (value - high.astype(F32)).astype(BF16)


def mul(a, b):
    (ah, al), (bh, bl) = a, b
    dot = functools.partial(jnp.dot, preferred_element_type=F32)
    return dot(ah, bh) + (dot(ah, bl) + dot(al, bh))


def cost(flops, nbytes):
    return pl.CostEstimate(flops=int(flops), bytes_accessed=int(nbytes), transcendentals=0)


def pack_kernel(core, v_ref, s_ref, keep_ref, send_ref, all_ref):
    span, width = v_ref.shape
    half, quarter = width // 2, width // 4
    part = keep_ref.shape[0]
    all_ref[:span] = v_ref[...]
    all_ref[span : span + half] = s_ref[:half]
    all_ref[span + half :, :half] = s_ref[half : half + quarter, half:]
    all_ref[span + half :, half:] = s_ref[half + quarter :, half:]
    me = core[0]
    keep_ref[...] = all_ref[pl.ds(pl.multiple_of(me * part, 8), part)]
    send_ref[...] = all_ref[pl.ds(pl.multiple_of((1 - me) * part, 8), part)]


def pack(core, v, s):
    span, width = v.shape
    part = (span + width // 2 + width // 4) // 2
    shape = jax.ShapeDtypeStruct((part, width), F32)
    return pl.pallas_call(
        pack_kernel,
        out_shape=(shape, shape),
        in_specs=[SMEM, VMEM, VMEM],
        out_specs=(VMEM, VMEM),
        scratch_shapes=[pltpu.VMEM((2 * part, width), F32)],
        cost_estimate=cost(1000, 4 * part * width * 4),
        compiler_params=LIMIT,
        name="pack",
    )(core, v, s)


def prepare_kernel(core, a_ref, b_ref, other_ref, th, tl, uh, ul, all_ref):
    width, span = th.shape
    half, quarter = width // 2, width // 4
    part, piece = other_ref.shape[0], a_ref.shape[0]
    me = core[0]
    mine = pl.multiple_of(me * part, 8)
    all_ref[pl.ds(mine, piece)] = a_ref[...]
    all_ref[pl.ds(pl.multiple_of(mine + piece, 8), piece)] = b_ref[...]
    all_ref[pl.ds(pl.multiple_of((1 - me) * part, 8), part)] = other_ref[...]
    v = all_ref[:span]
    top = all_ref[span : span + half]
    low = all_ref[span + half :]
    low = jnp.concatenate([low[:, :half], low[:, half:]], axis=0)
    s = jnp.concatenate([top, jnp.concatenate([jnp.zeros_like(low), low], axis=1)], axis=0)
    row = lax.broadcasted_iota(jnp.int32, s.shape, 0)
    column = lax.broadcasted_iota(jnp.int32, s.shape, 1)
    s = jnp.where(row <= column, s, 0.0)
    th[...], tl[...] = halves(v.T)
    uh[...], ul[...] = halves(mul(halves(v), halves(s)))


def prepare(core, a, b, other, span):
    part, width = other.shape
    tall = jax.ShapeDtypeStruct((span, width), BF16)
    wide = jax.ShapeDtypeStruct((width, span), BF16)
    return pl.pallas_call(
        prepare_kernel,
        out_shape=(wide, wide, tall, tall),
        in_specs=[SMEM, VMEM, VMEM, VMEM],
        out_specs=(VMEM,) * 4,
        scratch_shapes=[pltpu.VMEM((2 * part, width), F32)],
        cost_estimate=cost(6 * span * width * width, 16 * span * width),
        compiler_params=LIMIT,
        name="prepare",
    )(core, a, b, other)


def updated(window, th, tl, uh, ul):
    inner = mul((th[...], tl[...]), halves(window))
    return window - mul((uh[...], ul[...]), halves(inner))


def before_kernel(info, rest_in, lower_in, th, tl, uh, ul, rest, lower):
    width, span = th.shape
    slot, slots = info[0], info[2]
    rest[...] = rest_in[...]
    lower[...] = lower_in[...]

    @pl.when((slot > 0) & (slot < slots - 1))
    def _():
        at = pl.ds(pl.multiple_of((slot - 1) * width, width), span)
        rest[at] = updated(rest[at], th, tl, uh, ul)

    @pl.when(slot == slots - 1)
    def _():
        edge = rest.shape[0] - width
        window = jnp.concatenate([rest[edge:], lower[...]], axis=0)
        window = updated(window, th, tl, uh, ul)
        rest[edge:] = window[:width]
        lower[...] = window[width:]


def before(info, rest, lower, ops):
    width, span = ops[0].shape
    columns = rest.shape[1]
    return pl.pallas_call(
        before_kernel,
        out_shape=tuple(jax.ShapeDtypeStruct(x.shape, F32) for x in (rest, lower)),
        in_specs=[SMEM] + [VMEM] * 6,
        out_specs=(VMEM, VMEM),
        cost_estimate=cost(12 * span * width * columns, 8 * span * columns),
        compiler_params=LIMIT,
        name="before",
    )(info, rest, lower, *ops)


def after_kernel(info, rest_in, top_in, back, th, tl, uh, ul, rest, top):
    width = back.shape[0]
    rest[...] = rest_in[...]

    @pl.when(info[1] == 0)
    def _():
        top[...] = top_in[...]

    @pl.when(info[1] > 0)
    def _():
        top[...] = back[...]

    @pl.when(info[0] == 0)
    def _():
        window = jnp.concatenate([top[...], rest[:width]], axis=0)
        window = updated(window, th, tl, uh, ul)
        top[...] = window[:width]
        rest[:width] = window[width:]


def after(info, rest, top, back, ops):
    width, span = ops[0].shape
    columns = rest.shape[1]
    return pl.pallas_call(
        after_kernel,
        out_shape=tuple(jax.ShapeDtypeStruct(x.shape, F32) for x in (rest, top)),
        in_specs=[SMEM] + [VMEM] * 7,
        out_specs=(VMEM, VMEM),
        cost_estimate=cost(12 * span * width * columns, 8 * span * columns),
        compiler_params=LIMIT,
        name="after",
    )(info, rest, top, back, *ops)


def body(vectors, block_index, block_offset, reflector_vectors, reflector_factors):
    rows_here, columns_here = vectors.shape
    span, width = reflector_vectors.shape[2:]
    slots = rows_here // width
    owners, members = lax.axis_size("row"), lax.axis_size("vec")
    owner, member = lax.axis_index("row"), lax.axis_index("vec")
    bits = members.bit_length() - 1
    assert members == 1 << bits and bits > 0

    def swap(value, bit):
        return lax.ppermute(value, "vec", [(i, i ^ (1 << bit)) for i in range(members)])

    def to_above(value):
        return lax.ppermute(value, "row", [(i, i - 1) for i in range(1, owners)])

    def to_below(value):
        return lax.ppermute(value, "row", [(i, i + 1) for i in range(owners - 1)])

    core = jnp.reshape(member & 1, (1,)).astype(jnp.int32)
    keep, send = pack(core, reflector_vectors[0, 0], reflector_factors[0, 0])
    chunk = columns_here // CHUNKS
    cuts = [slice(j * chunk, (j + 1) * chunk) for j in range(CHUNKS)]
    top = [vectors[:width, cut] for cut in cuts]
    rest = [vectors[width:, cut] for cut in cuts]
    lower = [to_above(x) for x in top]
    received = swap(send, 0)
    piece = keep.shape[0] // 2

    def reflector(front):
        root = block_index[front, owner]

        def agrees(bit):
            return (root >> bit) & 1 == (member >> bit) & 1

        pieces = []
        for start, order in ((0, range(1, bits)), (piece, range(bits - 1, 0, -1))):
            at = slice(start, start + piece)
            value = jnp.where(agrees(0), keep[at], received[at])
            for bit in order:
                value = jnp.where(agrees(bit), value, swap(value, bit))
            pieces.append(value)
        other = swap(jnp.concatenate(pieces, axis=0), 0)
        return prepare(core, *pieces, other, span)

    ops = [reflector(front) for front in range(FRONTS)]
    for front in range(FRONTS):
        info = jnp.stack([block_offset[front, owner], owner, jnp.int32(slots)]).astype(jnp.int32)
        back = []
        for j in range(CHUNKS):
            rest[j], sent = before(info, rest[j], lower[j], ops[front])
            back.append(to_below(sent))
        for j in range(CHUNKS):
            rest[j], top[j] = after(info, rest[j], top[j], back[j], ops[front])
            if front < FRONTS - 1:
                lower[j] = to_above(top[j])
    return jnp.concatenate(
        [jnp.concatenate(top, axis=1), jnp.concatenate(rest, axis=1)], axis=0
    )


def solution(mesh):
    return jax.shard_map(
        body,
        mesh=mesh,
        in_specs=(
            P("row", "vec"),
            P(),
            P(),
            P("row", "vec", None, None),
            P("row", "vec", None, None),
        ),
        out_specs=P("row", "vec"),
        check_vma=False,
    )
```

```python
import functools

import jax
import jax.numpy as jnp
from jax import lax
from jax.experimental import pallas as pl
from jax.experimental.pallas import tpu as pltpu
from jax.sharding import PartitionSpec as P

FRONTS = 3
CHUNKS = 2


F32 = jnp.float32
BF16 = jnp.bfloat16
VMEM = pl.BlockSpec(memory_space=pltpu.VMEM)
LIMIT = pltpu.CompilerParams(vmem_limit_bytes=12 << 20)
SMEM = pl.BlockSpec(memory_space=pltpu.SMEM)


def halves(value):
    high = value.astype(BF16)
    return high, (value - high.astype(F32)).astype(BF16)


def mul(a, b):
    (ah, al), (bh, bl) = a, b
    dot = functools.partial(jnp.dot, preferred_element_type=F32)
    return dot(ah, bh) + (dot(ah, bl) + dot(al, bh))


def cost(flops, nbytes):
    return pl.CostEstimate(flops=int(flops), bytes_accessed=int(nbytes), transcendentals=0)


def member_bit(bit):
    return (lax.axis_index("vec") >> bit) & 1


def pack_kernel(v_ref, s_ref, keep_ref, send_ref, all_ref):
    span, width = v_ref.shape
    half, quarter = width // 2, width // 4
    part = keep_ref.shape[0]
    all_ref[:span] = v_ref[...]
    all_ref[span : span + half] = s_ref[:half]
    all_ref[span + half :, :half] = s_ref[half : half + quarter, half:]
    all_ref[span + half :, half:] = s_ref[half + quarter :, half:]
    me = member_bit(0)
    keep_ref[...] = all_ref[pl.ds(pl.multiple_of(me * part, 8), part)]
    send_ref[...] = all_ref[pl.ds(pl.multiple_of((1 - me) * part, 8), part)]


def pack(v, s):
    span, width = v.shape
    part = (span + width // 2 + width // 4) // 2
    shape = jax.ShapeDtypeStruct((part, width), F32)
    return pl.pallas_call(
        pack_kernel,
        out_shape=(shape, shape),
        in_specs=[VMEM, VMEM],
        out_specs=(VMEM, VMEM),
        scratch_shapes=[pltpu.VMEM((2 * part, width), F32)],
        cost_estimate=cost(1000, 4 * part * width * 4),
        compiler_params=LIMIT,
        name="pack",
    )(v, s)


def choose_kernel(jobs, index, *refs):
    owner = lax.axis_index("row")
    for front, bit, own, other, out in jobs:
        rows = refs[out].shape[0]
        agrees = ((index[front, owner] >> bit) & 1) == member_bit(bit)

        @pl.when(agrees)
        def _():
            refs[out][...] = refs[own[0]][own[1] : own[1] + rows]

        @pl.when(jnp.logical_not(agrees))
        def _():
            refs[out][...] = refs[other[0]][other[1] : other[1] + rows]


def choose(index, sources, jobs, rows, name):
    count, width = len(sources), sources[0].shape[1]
    numbered = [job + (count + i,) for i, job in enumerate(jobs)]
    return pl.pallas_call(
        functools.partial(choose_kernel, numbered),
        out_shape=tuple(jax.ShapeDtypeStruct((rows, width), F32) for _ in jobs),
        in_specs=[SMEM] + [VMEM] * count,
        out_specs=(VMEM,) * len(jobs),
        cost_estimate=cost(1000, 8 * rows * width * len(jobs)),
        compiler_params=LIMIT,
        name=name,
    )(index, *sources)


def prepare_kernel(a_ref, b_ref, other_ref, th, tl, uh, ul, all_ref):
    width, span = th.shape
    half, quarter = width // 2, width // 4
    part, piece = other_ref.shape[0], a_ref.shape[0]
    me = member_bit(0)
    mine = pl.multiple_of(me * part, 8)
    all_ref[pl.ds(mine, piece)] = a_ref[...]
    all_ref[pl.ds(pl.multiple_of(mine + piece, 8), piece)] = b_ref[...]
    all_ref[pl.ds(pl.multiple_of((1 - me) * part, 8), part)] = other_ref[...]
    v = all_ref[:span]
    top = all_ref[span : span + half]
    low = all_ref[span + half :]
    low = jnp.concatenate([low[:, :half], low[:, half:]], axis=0)
    s = jnp.concatenate([top, jnp.concatenate([jnp.zeros_like(low), low], axis=1)], axis=0)
    row = lax.broadcasted_iota(jnp.int32, s.shape, 0)
    column = lax.broadcasted_iota(jnp.int32, s.shape, 1)
    s = jnp.where(row <= column, s, 0.0)
    th[...], tl[...] = halves(v.T)
    uh[...], ul[...] = halves(mul(halves(v), halves(s)))


def prepare(a, b, other, span):
    part, width = other.shape
    tall = jax.ShapeDtypeStruct((span, width), BF16)
    wide = jax.ShapeDtypeStruct((width, span), BF16)
    return pl.pallas_call(
        prepare_kernel,
        out_shape=(wide, wide, tall, tall),
        in_specs=[VMEM, VMEM, VMEM],
        out_specs=(VMEM,) * 4,
        scratch_shapes=[pltpu.VMEM((2 * part, width), F32)],
        cost_estimate=cost(6 * span * width * width, 16 * span * width),
        compiler_params=LIMIT,
        name="prepare",
    )(a, b, other)


def updated(window, th, tl, uh, ul):
    inner = mul((th[...], tl[...]), halves(window))
    return window - mul((uh[...], ul[...]), halves(inner))


def before_kernel(front, rest_at, lower_at, slots, offset, rest_in, lower_in, th, tl, uh, ul, rest, lower):
    width, span = th.shape
    slot = offset[front, lax.axis_index("row")]
    rest[...] = rest_in[rest_at]
    lower[...] = lower_in[lower_at]

    @pl.when((slot > 0) & (slot < slots - 1))
    def _():
        at = pl.ds(pl.multiple_of((slot - 1) * width, width), span)
        rest[at] = updated(rest[at], th, tl, uh, ul)

    @pl.when(slot == slots - 1)
    def _():
        edge = rest.shape[0] - width
        window = jnp.concatenate([rest[edge:], lower[...]], axis=0)
        window = updated(window, th, tl, uh, ul)
        rest[edge:] = window[:width]
        lower[...] = window[width:]


def before(front, slots, chunk, offset, rest, lower, ops):
    width, span = ops[0].shape
    shapes = ((slots - 1) * width, chunk), (width, chunk)
    return pl.pallas_call(
        functools.partial(before_kernel, front, rest[1], lower[1], slots),
        out_shape=tuple(jax.ShapeDtypeStruct(shape, F32) for shape in shapes),
        in_specs=[SMEM] + [VMEM] * 6,
        out_specs=(VMEM, VMEM),
        cost_estimate=cost(12 * span * width * chunk, 8 * span * chunk),
        compiler_params=LIMIT,
        name="before",
    )(offset, rest[0], lower[0], *ops)


def after_kernel(front, top_at, final, offset, rest_in, top_in, back, th, tl, uh, ul, *out):
    width = back.shape[0]
    owner = lax.axis_index("row")
    if final:
        top, rest = out[-1].at[:width], out[-1].at[width:]
    else:
        rest, top = out
    rest[...] = rest_in[...]

    @pl.when(owner == 0)
    def _():
        top[...] = top_in[top_at]

    @pl.when(owner > 0)
    def _():
        top[...] = back[...]

    @pl.when(offset[front, owner] == 0)
    def _():
        window = jnp.concatenate([top[...], rest[:width]], axis=0)
        window = updated(window, th, tl, uh, ul)
        top[...] = window[:width]
        rest[:width] = window[width:]


def after(front, offset, rest, top, back, ops, final=None):
    width, span = ops[0].shape
    columns = rest.shape[1]
    out_shape = tuple(jax.ShapeDtypeStruct((rows, columns), F32) for rows in (rest.shape[0], width))
    out_specs = (VMEM, VMEM)
    arrays, specs, aliases, grid = [], [], {}, ()
    if final is not None:
        shape, block, so_far = final
        grid = (1,)
        out_shape = jax.ShapeDtypeStruct(shape, F32)
        out_specs = pl.BlockSpec((shape[0], columns), lambda i: (0, block))
        if so_far is not None:
            arrays, specs, aliases = [so_far], [pl.BlockSpec(memory_space=pl.ANY)], {8: 0}
    return pl.pallas_call(
        functools.partial(after_kernel, front, top[1], final is not None),
        out_shape=out_shape,
        grid=grid,
        in_specs=[SMEM] + [VMEM] * 7 + specs,
        out_specs=out_specs,
        input_output_aliases=aliases,
        cost_estimate=cost(12 * span * width * columns, 8 * span * columns),
        compiler_params=LIMIT,
        name="after",
    )(offset, rest, top[0], back, *ops, *arrays)


def body(vectors, block_index, block_offset, reflector_vectors, reflector_factors):
    rows_here, columns_here = vectors.shape
    span, width = reflector_vectors.shape[2:]
    slots = rows_here // width
    owners, members = lax.axis_size("row"), lax.axis_size("vec")
    bits = members.bit_length() - 1
    assert members == 1 << bits and bits > 1

    def swap(value, bit):
        return lax.ppermute(value, "vec", [(i, i ^ (1 << bit)) for i in range(members)])

    def to_above(value):
        return lax.ppermute(value, "row", [(i, i - 1) for i in range(1, owners)])

    def to_below(value):
        return lax.ppermute(value, "row", [(i, i + 1) for i in range(owners - 1)])

    keep, send = pack(reflector_vectors[0, 0], reflector_factors[0, 0])
    received = swap(send, 0)
    lower_rows = to_above(vectors[:width])
    piece = keep.shape[0] // 2
    orders = tuple(range(1, bits)), tuple(range(bits - 1, 0, -1))

    def first(fronts, extra=()):
        jobs = [(f, 0, (0, at), (1, at)) for f in fronts for at in (0, piece)]
        more = [(f, bit, (2 + 2 * i, 0), (3 + 2 * i, 0)) for i, (f, bit, _, _) in enumerate(extra)]
        sources = [keep, received] + [x for e in extra for x in e[2:]]
        out = choose(block_index, sources, more + jobs, piece, "choose")
        return out[: len(more)], out[len(more) :]

    held = {}
    _, start = first(tuple(range(min(2, FRONTS))))
    for f in range(min(2, FRONTS)):
        held[f] = list(start[2 * f : 2 * f + 2])
    ops = []
    for f in range(FRONTS):
        for step in range(bits - 1):
            came = [swap(held[f][side], orders[side][step]) for side in (0, 1)]
            extra = [(f, orders[side][step], held[f][side], came[side]) for side in (0, 1)]
            ahead = f + 1 if step == 0 and 2 <= f + 1 < FRONTS else None
            done, start = first(() if ahead is None else (ahead,), extra)
            held[f] = list(done)
            if ahead is not None:
                held[ahead] = list(start)
        other = swap(jnp.concatenate(held[f], axis=0), 0)
        ops.append(prepare(*held[f], other, span))

    chunk = columns_here // CHUNKS
    cuts = [slice(j * chunk, (j + 1) * chunk) for j in range(CHUNKS)]
    every = (slice(None), slice(None))
    rest = [(vectors, (slice(width, None), cut)) for cut in cuts]
    top = [(vectors, (slice(0, width), cut)) for cut in cuts]
    lower = [(lower_rows, (slice(None), cut)) for cut in cuts]
    whole = None
    for front in range(FRONTS):
        back = []
        for j in range(CHUNKS):
            kept, sent = before(front, slots, chunk, block_offset, rest[j], lower[j], ops[front])
            rest[j] = kept
            back.append(to_below(sent))
        for j in range(CHUNKS):
            if front == FRONTS - 1:
                final = (vectors.shape, j, whole)
                whole = after(front, block_offset, rest[j], top[j], back[j], ops[front], final)
                continue
            kept, top_j = after(front, block_offset, rest[j], top[j], back[j], ops[front])
            lower[j] = (to_above(top_j), every)
            rest[j], top[j] = (kept, every), (top_j, every)
    return whole


def solution(mesh):
    return jax.shard_map(
        body,
        mesh=mesh,
        in_specs=(
            P("row", "vec"),
            P(),
            P(),
            P("row", "vec", None, None),
            P("row", "vec", None, None),
        ),
        out_specs=P("row", "vec"),
        check_vma=False,
    )
```
